256 devices in a mesh: rep: 1, r: 4 (over x), s: 64 (over y, z, core).
Axes of the slice: x: 4, y: 4, z: 8, core: 2. Of those that a mesh axis runs over, the one named last changes fastest.
Arguments:
- x: bfloat16 [256, 2048, 640], P(('rep', 'r', 's'))
- dy: bfloat16 [256, 2048, 640], P(('rep', 'r', 's'))
- w_gate: bfloat16 [2, 640, 2560], P(None, 's')
- w_up: bfloat16 [2, 640, 2560], P(None, 's')
- w_down: bfloat16 [2, 2560, 640], P(None, 's')
Outputs:
- output 1: bfloat16 [256, 2048, 640], P(('rep', 'r', 's'))
- output 2: bfloat16 [2, 640, 2560], P('rep', 's')
- output 3: bfloat16 [2, 640, 2560], P('rep', 's')
- output 4: bfloat16 [2, 2560, 640], P('rep', 's')
All inputs are finite; a program needn't handle non-finite values.
Results may differ from the reference program's by a relative error of at most 0.018.
Values are sent between devices in bfloat16 or wider.
A program may use at most 768 MiB of HBM per device.

```python
import jax
import jax.numpy as jnp
from jax import lax

SEQUENCES = 256
TOKENS = 2048
D = 640
FF = 2560
LAYERS = 2
NAMES = ("w_gate", "w_up", "w_down")
SHAPES = {"w_gate": (LAYERS, D, FF), "w_up": (LAYERS, D, FF), "w_down": (LAYERS, FF, D)}


def bump(key, n, height):
    away = (jnp.arange(n, dtype=jnp.int32) - jax.random.randint(key, (), 0, n, jnp.int32)) % n
    return jnp.where(away < n // 8, height, 1.0)


def together(key, own, strength):
    shared = jax.random.normal(key, own.shape[1:], jnp.float32)
    return (own + strength * shared) * lax.rsqrt(1 + strength * strength)


def setup_inputs(seed: int = 0, part: int = 0) -> dict:
    kx, kdy, ka, kb, kz, kf, kh, kl, *kw = jax.random.split(jax.random.key(seed), 8 + len(NAMES))
    kx, kdy, ka, kb = (jax.random.fold_in(k, part) for k in (kx, kdy, ka, kb))
    shape = (SEQUENCES, TOKENS, D)
    much_x, much_dy = jax.random.uniform(kz, (2,), jnp.float32, 0.0, 1.0)
    layers = 2.0 ** jax.random.uniform(kl, (LAYERS, 1, 1), jnp.float32, -1.0, 1.0)
    x = together(ka, jax.random.normal(kx, shape, jnp.float32), much_x) * bump(kf, D, 4.0)
    dy = together(kb, jax.random.normal(kdy, shape, jnp.float32), much_dy)
    drawn = {"x": x.astype(jnp.bfloat16), "dy": (dy * (SEQUENCES * TOKENS) ** -0.5).astype(jnp.bfloat16)}
    for key, name in zip(kw, NAMES, strict=True):
        w = jax.random.normal(key, SHAPES[name], jnp.float32) * SHAPES[name][1] ** -0.5
        drawn[name] = (w * {"w_gate": 1.0, "w_up": bump(kh, FF, 4.0), "w_down": layers}[name]).astype(jnp.bfloat16)
    return drawn


def matmul(a, w):
    return jnp.dot(a, w, preferred_element_type=jnp.float32).astype(jnp.bfloat16)


def normed(h):
    wide = h.astype(jnp.float32)
    scale = lax.rsqrt(jnp.mean(wide**2, -1, keepdims=True) + 1e-6)
    return (wide * scale).astype(jnp.bfloat16)


def layer(h, w):
    a = normed(h)
    gate = jnp.dot(a, w["w_gate"], preferred_element_type=jnp.float32)
    up = jnp.dot(a, w["w_up"], preferred_element_type=jnp.float32)
    return h + matmul((jax.nn.silu(gate) * up).astype(jnp.bfloat16), w["w_down"])


def stack(weights, h):
    return lax.scan(lambda h, w: (layer(h, w), None), h, weights)[0]


def reference(x, dy, w_gate, w_up, w_down):
    weights = dict(zip(NAMES, (w_gate, w_up, w_down), strict=True))

    def take(so_far, sequence):
        h, by_y = sequence
        _, back = jax.vjp(stack, weights, h)
        by_weights, by_h = back(by_y)
        return jax.tree.map(lambda total, term: total + term.astype(jnp.float32), so_far, by_weights), by_h

    none_yet = {name: jnp.zeros(w.shape, jnp.float32) for name, w in weights.items()}
    by_weights, by_x = lax.scan(take, none_yet, (x, dy))
    return (by_x, *(by_weights[name].astype(jnp.bfloat16) for name in NAMES))
```

```python
import functools

import jax
import jax.numpy as jnp
from jax import lax
from jax.experimental import pallas as pl
from jax.experimental.pallas import tpu as pltpu
from jax.sharding import PartitionSpec as P

NAMES = ("w_gate", "w_up", "w_down")
ROWS = 128
NY, NZ = 4, 8


def matmul(a, w):
    return jnp.dot(a, w, preferred_element_type=jnp.float32).astype(jnp.bfloat16)


def normed(h):
    wide = h.astype(jnp.float32)
    scale = lax.rsqrt(jnp.mean(wide**2, -1, keepdims=True) + 1e-6)
    return (wide * scale).astype(jnp.bfloat16)


def layer(h, w):
    a = normed(h)
    gate = jnp.dot(a, w["w_gate"], preferred_element_type=jnp.float32)
    up = jnp.dot(a, w["w_up"], preferred_element_type=jnp.float32)
    return h + matmul((jax.nn.silu(gate) * up).astype(jnp.bfloat16), w["w_down"])


def place(ny, nz):
    s = lax.axis_index("s")
    return s // (2 * nz), lax.rem(s // 2, nz), lax.rem(s, 2)


def greet(peers):
    barrier = pltpu.get_barrier_semaphore()
    for peer in peers:
        pl.semaphore_signal(barrier, inc=1, device_id=peer, device_id_type=pl.DeviceIdType.MESH)
    pl.semaphore_wait(barrier, len(peers))


def remote(src, dst, send, recv, peer):
    return pltpu.make_async_remote_copy(
        src_ref=src, dst_ref=dst, send_sem=send, recv_sem=recv, device_id=peer, device_id_type=pl.DeviceIdType.MESH
    )


def ring(axis, y, z, c, ny, nz):
    n, pos = (ny, y) if axis == "y" else (nz, z)

    def at(k):
        return {"s": ((k * nz + z) if axis == "y" else (y * nz + k)) * 2 + c}

    return n, pos, (at(lax.rem(pos + 1, n)), at(lax.rem(pos + n - 1, n)))


def gather_kernel(ny, nz, w_ref, o_ref, own_sem, pair_send, pair_recv, send1, recv1, send2, recv2):
    rows = w_ref.shape[0]
    half = rows // 2
    y, z, c = place(ny, nz)
    partner = {"s": (y * nz + z) * 2 + (1 - c)}
    peers = [partner, *ring("y", y, z, c, ny, nz)[2], *ring("z", y, z, c, ny, nz)[2]]
    greet(peers)
    own = pltpu.make_async_copy(w_ref, o_ref.at[y, z, c], own_sem)
    own.start()
    own.wait()

    def hand(ref):
        remote(ref, ref, pair_send, pair_recv, partner).start()

    hand(o_ref.at[y, z, c])

    def phase(axis, block, subs, send, recv):
        n, pos, to = ring(axis, y, z, c, ny, nz)
        h = n // 2
        sent = []

        def piece(k, j, which):
            ref = block(k, j)
            return ref if which is None else ref.at[pl.ds(which * half, half)]

        def copy(d, t, j):
            origin = lax.rem(pos + n - t, n) if d == 0 else lax.rem(pos + t, n)
            ref = piece(origin, j, d if t == h - 1 else None)
            return remote(ref, ref, send.at[d, t, j], recv.at[d, t, j], to[d])

        def arrived(d, t, j):
            origin = lax.rem(pos + n - t - 1, n) if d == 0 else lax.rem(pos + t + 1, n)
            ref = piece(origin, j, d if t == h - 1 else None)
            remote(ref, ref, send.at[d, t, j], recv.at[d, t, j], to[d]).wait_recv()
            return ref

        for t in range(h):
            for j in range(subs):
                for d in (0, 1):
                    ref = arrived(d, t - 1, j) if t else None
                    sent.append(copy(d, t, j))
                    sent[-1].start()
                    if t:
                        hand(ref)
        for j in range(subs):
            for d in (0, 1):
                hand(arrived(d, h - 1, j))
        return sent

    @pl.when(c == 0)
    def _():
        sent = phase("y", lambda k, j: o_ref.at[k, z, c], 1, send1, recv1)
        sent += phase("z", lambda k, j: o_ref.at[j, k, c], ny, send2, recv2)
        for copy in sent:
            copy.wait_send()

    @pl.when(c == 1)
    def _():
        sent = phase("z", lambda k, j: o_ref.at[y, k, c], 1, send1, recv1)
        sent += phase("y", lambda k, j: o_ref.at[k, j, c], nz, send2, recv2)
        for copy in sent:
            copy.wait_send()

    remote(o_ref.at[:, :, c], o_ref.at[:, :, c], pair_send, pair_recv, partner).wait_send()
    remote(o_ref.at[:, :, 1 - c], o_ref.at[:, :, 1 - c], pair_send, pair_recv, partner).wait_recv()


def gathered(block, ny=NY, nz=NZ, interpret=False):
    rows, width = block.shape
    dma = pltpu.SemaphoreType.DMA
    return pl.pallas_call(
        functools.partial(gather_kernel, ny, nz),
        out_shape=jax.ShapeDtypeStruct((ny, nz, 2, rows, width), block.dtype),
        in_specs=[pl.BlockSpec(memory_space=pltpu.VMEM)],
        out_specs=pl.BlockSpec(memory_space=pl.ANY),
        scratch_shapes=[dma, dma, dma, dma((2, 4, 1)), dma((2, 4, 1)), dma((2, 4, 8)), dma((2, 4, 8))],
        compiler_params=pltpu.CompilerParams(collective_id=1, has_side_effects=True),
        cost_estimate=pl.CostEstimate(flops=20_000_000_000, bytes_accessed=10_000_000, transcendentals=0),
        name="gather_plane",
    )(block)


def reduce_kernel(nx, ny, nz, g_ref, b_ref, o1_ref, o2_ref, mine, theirs, arrivals1, arrivals2, copies1, copies2, own_sem,
                  pair_send, pair_recv, send1, recv1, send2, recv2, xsend, xrecv):
    rows = b_ref.shape[0]
    half = rows // 2
    tile = min(rows // 2, 64)
    x = lax.axis_index("r")
    y, z, c = place(ny, nz)
    partner = {"s": (y * nz + z) * 2 + (1 - c)}
    planes = [{"r": lax.rem(x + k, nx)} for k in range(1, nx)]
    greet([partner, *ring("y", y, z, c, ny, nz)[2], *ring("z", y, z, c, ny, nz)[2], *planes])
    own = pltpu.make_async_copy(g_ref.at[:, :, c], mine, own_sem)
    own.start()

    def pair(yy, zz, core):
        i = yy * nz + zz
        return remote(g_ref.at[yy, zz, core], theirs.at[yy, zz], pair_send.at[i], pair_recv.at[i], partner)

    def needed(n, pos):
        h = n // 2
        offsets = [h]
        for t in range(1, h):
            offsets += [h - t, n - h + t]
        return [lax.rem(pos + k, n) for k in [*offsets, 0]]

    @pl.when(c == 0)
    def _():
        for k in needed(ny, y):
            for j in range(nz):
                pair(k, j, 1).start()

    @pl.when(c == 1)
    def _():
        for k in needed(nz, z):
            for j in range(ny):
                pair(j, k, 0).start()

    def spread(layer, source, copies):
        return [
            remote(source, copies.at[x], xsend.at[layer, k], xrecv.at[layer, k], peer) for k, peer in enumerate(planes)
        ]

    def add(into, block, first=0, count=rows):
        def body(i, _):
            at = pl.ds(pl.multiple_of(first + i * tile, tile), tile)
            into[at, :] = (into[at, :].astype(jnp.float32) + block[at, :].astype(jnp.float32)).astype(into.dtype)
            return 0

        lax.fori_loop(0, count // tile, body, 0)

    def keep(into, block):
        def body(i, _):
            at = pl.ds(pl.multiple_of(i * tile, tile), tile)
            into[at, :] = block[at, :]
            return 0

        lax.fori_loop(0, rows // tile, body, 0)

    def over_planes(out, copies):
        def body(i, _):
            at = pl.ds(pl.multiple_of(i * tile, tile), tile)
            total = copies[0, at, :].astype(jnp.float32)
            for k in range(1, nx):
                total += copies[k, at, :].astype(jnp.float32)
            out[at, :] = total.astype(out.dtype)
            return 0

        lax.fori_loop(0, rows // tile, body, 0)

    other = spread(1, b_ref, copies2)
    for copy in other:
        copy.start()
    keep(copies2.at[x], b_ref)
    own.wait()

    def both(yy, zz):
        pair(yy, zz, 1 - c).wait_recv()
        add(mine.at[yy, zz], theirs.at[yy, zz])

    def phase(axis, block, subs, ready, arrivals, send, recv):
        n, pos, to = ring(axis, y, z, c, ny, nz)
        h = n // 2
        sent = []

        def rows_of(ref, d, t):
            return ref.at[pl.ds(d * half, half)] if t == 0 else ref

        def arrived(d, t, j, into):
            landed = arrivals.at[d, t * subs + j]
            part = rows_of(landed, d, t)
            remote(part, part, send.at[d, t, j], recv.at[d, t, j], to[d]).wait_recv()
            add(into, landed, d * half if t == 0 else 0, half if t == 0 else rows)

        for t in range(h):
            for j in range(subs):
                for d in (0, 1):
                    k = lax.rem(pos + h - t, n) if d == 0 else lax.rem(pos + n - h + t, n)
                    if t or d == 0:
                        ready(k, j)
                    if t:
                        arrived(d, t - 1, j, block(k, j))
                    sent.append(
                        remote(
                            rows_of(block(k, j), d, t), rows_of(arrivals.at[d, t * subs + j], d, t),
                            send.at[d, t, j], recv.at[d, t, j], to[d],
                        )
                    )
                    sent[-1].start()
        for j in range(subs):
            ready(pos, j)
            for d in (0, 1):
                arrived(d, h - 1, j, block(pos, j))
        return sent

    def done(k, j):
        pass

    @pl.when(c == 0)
    def _():
        sent = phase("z", lambda k, j: mine.at[j, k], ny, lambda k, j: both(j, k), arrivals1, send1, recv1)
        sent += phase("y", lambda k, j: mine.at[k, z], 1, done, arrivals2, send2, recv2)
        for copy in sent:
            copy.wait_send()

    @pl.when(c == 1)
    def _():
        sent = phase("y", lambda k, j: mine.at[k, j], nz, lambda k, j: both(k, j), arrivals1, send1, recv1)
        sent += phase("z", lambda k, j: mine.at[y, k], 1, done, arrivals2, send2, recv2)
        for copy in sent:
            copy.wait_send()

    last = spread(0, mine.at[y, z], copies1)
    for copy in last:
        copy.start()
    keep(copies1.at[x], mine.at[y, z])
    for copy in other:
        copy.wait()
    over_planes(o2_ref, copies2)
    for copy in last:
        copy.wait()
    over_planes(o1_ref, copies1)
    for yy in range(ny):
        for zz in range(nz):
            pair(yy, zz, 1 - c).wait_send()


def reduced(grads, block, nx, ny=NY, nz=NZ):
    rows, width = block.shape
    dma = pltpu.SemaphoreType.DMA
    vmem = lambda *lead: pltpu.VMEM((*lead, rows, width), jnp.bfloat16)
    one = jax.ShapeDtypeStruct((rows, width), jnp.bfloat16)
    return pl.pallas_call(
        functools.partial(reduce_kernel, nx, ny, nz),
        out_shape=(one, one),
        in_specs=[pl.BlockSpec(memory_space=pl.ANY), pl.BlockSpec(memory_space=pltpu.VMEM)],
        out_specs=(pl.BlockSpec(memory_space=pltpu.VMEM),) * 2,
        scratch_shapes=[
            vmem(ny, nz), vmem(ny, nz), vmem(2, ny * nz // 2), vmem(2, max(ny, nz) // 2), vmem(nx), vmem(nx),
            dma, dma((ny * nz,)), dma((ny * nz,)),
            dma((2, 4, 8)), dma((2, 4, 8)), dma((2, 4, 1)), dma((2, 4, 1)), dma((2, max(nx - 1, 1))), dma((2, max(nx - 1, 1))),
        ],
        compiler_params=pltpu.CompilerParams(collective_id=2, has_side_effects=True, vmem_limit_bytes=40 * 2**20),
        cost_estimate=pl.CostEstimate(flops=40_000_000_000, bytes_accessed=20_000_000, transcendentals=0),
        name="reduce_all",
    )(grads, block)


def solution(mesh):
    nx = mesh.shape["r"]
    shards = mesh.shape["s"]

    def packed(weights, number):
        return jnp.concatenate([w[number].reshape(-1, 640) for w in weights], axis=0)

    def padded(block):
        return jnp.pad(block, ((0, ROWS - block.shape[0]), (0, 0)))

    def matrices(blocks):
        gate, up, down = (blocks[:, 40 * i : 40 * i + 40] for i in range(3))
        return {"w_gate": gate.reshape(640, 2560), "w_up": up.reshape(640, 2560), "w_down": down.reshape(2560, 640)}

    def terms(by_w, pad):
        parts = [by_w[name].reshape(shards, 40, 640) for name in NAMES]
        if pad:
            parts.append(jnp.zeros((shards, ROWS - 120, 640), jnp.bfloat16))
        return jnp.concatenate(parts, axis=1)

    def step(x, dy, *weights):
        blocks = lax.all_gather(packed(weights, 1), "s", axis=0, tiled=True)
        first = gathered(padded(packed(weights, 0))).reshape(shards, ROWS, 640)
        h0 = x[0]
        w0 = matrices(first)
        h1 = layer(h0, w0)
        w1 = matrices(blocks.reshape(shards, 120, 640))
        _, back = jax.vjp(lambda w, h: layer(h, w), w1, h1)
        by_w, by_h = back(dy[0])
        second = lax.psum_scatter(terms(by_w, False).reshape(-1, 640), "s", scatter_dimension=0, tiled=True)
        w0, h0, by_h = lax.optimization_barrier((w0, h0, by_h))
        _, back = jax.vjp(lambda w, h: layer(h, w), w0, h0)
        by_w, by_x = back(by_h)
        one, two = reduced(terms(by_w, True).reshape(NY, NZ, 2, ROWS, 640), padded(second), nx)
        both = jnp.stack([one, two])
        mine = [both[:, :40].reshape(2, 10, 2560), both[:, 40:80].reshape(2, 10, 2560), both[:, 80:120]]
        return (by_x[None], *mine)

    states, cut = P(("rep", "r", "s"), None, None), P(None, "s", None)
    return jax.shard_map(
        step,
        mesh=mesh,
        in_specs=(states, states) + (cut,) * 3,
        out_specs=(states,) + (P("rep", "s", None),) * 3,
        check_vma=False,
    )
```

```python
import functools

import jax
import jax.numpy as jnp
from jax import lax
from jax.experimental import pallas as pl
from jax.experimental.pallas import tpu as pltpu
from jax.sharding import PartitionSpec as P

NY, NZ = 4, 8
EDGE = 16


def scale_of(wide):
    return lax.rsqrt(jnp.mean(wide**2, -1, keepdims=True) + 1e-6)


def dot(a, b):
    return jnp.dot(a, b, preferred_element_type=jnp.float32)


def dot_t(a, b):
    return lax.dot_general(a, b, (((1,), (1,)), ((), ())), preferred_element_type=jnp.float32)


def tiles(count, size, body):
    def run(i, _):
        body(pl.ds(pl.multiple_of(i * size, size), size))
        return 0

    lax.fori_loop(0, count // size, run, 0)


def forward_kernel(steps, tile, h_ref, g_ref, u_ref, d_ref, y_ref, a_ref, total):
    q = pl.program_id(0)
    tokens = h_ref.shape[0]

    @pl.when(q == 0)
    def _():
        def start(at):
            wide = h_ref[at, :].astype(jnp.float32)
            a_ref[at, :] = (wide * scale_of(wide)).astype(jnp.bfloat16)
            total[at, :] = jnp.zeros((tile, h_ref.shape[1]), jnp.float32)

        tiles(tokens, tile, start)

    def main(at):
        a = a_ref[at, :]
        gate, up = dot(a, g_ref[...]), dot(a, u_ref[...])
        act = (gate * jax.nn.sigmoid(gate) * up).astype(jnp.bfloat16)
        total[at, :] += dot(act, d_ref[...])

    tiles(tokens, tile, main)

    @pl.when(q == steps - 1)
    def _():
        def end(at):
            y_ref[at, :] = h_ref[at, :] + total[at, :].astype(jnp.bfloat16)

        tiles(tokens, tile, end)


def forward(h, number, both, down, tile=512):
    tokens, d = h.shape
    steps = both.shape[2] // d
    whole = pl.BlockSpec((tokens, d), lambda q: (0, 0))
    gate_at = pl.BlockSpec((None, d, d), lambda q: (2 * number, 0, q))
    up_at = pl.BlockSpec((None, d, d), lambda q: (2 * number + 1, 0, q))
    down_at = pl.BlockSpec((None, d, d), lambda q: (number, q, 0))
    return pl.pallas_call(
        functools.partial(forward_kernel, steps, tile),
        grid=(steps,),
        out_shape=jax.ShapeDtypeStruct((tokens, d), jnp.bfloat16),
        in_specs=[whole, gate_at, up_at, down_at],
        out_specs=whole,
        scratch_shapes=[pltpu.VMEM((tokens, d), jnp.bfloat16), pltpu.VMEM((tokens, d), jnp.float32)],
        compiler_params=pltpu.CompilerParams(dimension_semantics=("arbitrary",), vmem_limit_bytes=48 * 2**20),
        cost_estimate=pl.CostEstimate(flops=20_000_000_000, bytes_accessed=15_000_000, transcendentals=5_000_000),
        name="layer_forward",
    )(h, both, both, down)


def backward_kernel(steps, tile, h_ref, dy_ref, g_ref, u_ref, d_ref, by_both, by_d, by_h,
                    a_ref, at_ref, dyt_ref, act_ref, dgate_ref, dup_ref, total_g, total_u):
    q = pl.program_id(0)
    tokens, d = h_ref.shape

    @pl.when(q == 0)
    def _():
        def start(at):
            wide = h_ref[at, :].astype(jnp.float32)
            a = (wide * scale_of(wide)).astype(jnp.bfloat16)
            a_ref[at, :] = a
            at_ref[:, at] = a.T
            dyt_ref[:, at] = dy_ref[at, :].T
            total_g[at, :] = jnp.zeros((tile, d), jnp.float32)
            total_u[at, :] = jnp.zeros((tile, d), jnp.float32)

        tiles(tokens, tile, start)

    def main(at):
        a = a_ref[at, :]
        gate, up = dot(a, g_ref[...]), dot(a, u_ref[...])
        dact = dot_t(dy_ref[at, :], d_ref[...]).astype(jnp.bfloat16).astype(jnp.float32)
        s = jax.nn.sigmoid(gate)
        silu = gate * s
        act_ref[at, :] = (silu * up).astype(jnp.bfloat16)
        dup = (dact * silu).astype(jnp.bfloat16)
        dgate = (dact * up * (s + silu * (1.0 - s))).astype(jnp.bfloat16)
        dup_ref[at, :] = dup
        dgate_ref[at, :] = dgate
        total_g[at, :] += dot_t(dgate, g_ref[...])
        total_u[at, :] += dot_t(dup, u_ref[...])

    tiles(tokens, tile, main)

    by_d[...] = dot(dyt_ref[...], act_ref[...]).T.astype(jnp.bfloat16)
    by_both[0] = dot(at_ref[...], dgate_ref[...]).astype(jnp.bfloat16)
    by_both[1] = dot(at_ref[...], dup_ref[...]).astype(jnp.bfloat16)

    @pl.when(q == steps - 1)
    def _():
        def end(at):
            wide = h_ref[at, :].astype(jnp.float32)
            scale = scale_of(wide)
            da = (total_g[at, :].astype(jnp.bfloat16) + total_u[at, :].astype(jnp.bfloat16)).astype(jnp.float32)
            along = jnp.sum(da * wide, -1, keepdims=True) * (scale * scale * scale) * (1.0 / d)
            by_h[at, :] = dy_ref[at, :] + (da * scale - wide * along).astype(jnp.bfloat16)

        tiles(tokens, tile, end)


def backward(h, dy, number, both, down, tile=512):
    tokens, d = h.shape
    steps = both.shape[2] // d
    whole = pl.BlockSpec((tokens, d), lambda q: (0, 0))
    gate_at = pl.BlockSpec((None, d, d), lambda q: (2 * number, 0, q))
    up_at = pl.BlockSpec((None, d, d), lambda q: (2 * number + 1, 0, q))
    down_at = pl.BlockSpec((None, d, d), lambda q: (number, q, 0))
    like = lambda v, count: jax.ShapeDtypeStruct((count, *v.shape[1:]), v.dtype)
    state = lambda t: pltpu.VMEM((tokens, d), t)
    flat = lambda: pltpu.VMEM((d, tokens), jnp.bfloat16)
    return pl.pallas_call(
        functools.partial(backward_kernel, steps, tile),
        grid=(steps,),
        out_shape=(like(both, 2), like(down, 1), jax.ShapeDtypeStruct(h.shape, h.dtype)),
        in_specs=[whole, whole, gate_at, up_at, down_at],
        out_specs=(pl.BlockSpec((2, d, d), lambda q: (0, 0, q)), pl.BlockSpec((None, d, d), lambda q: (0, q, 0)), whole),
        scratch_shapes=[
            state(jnp.bfloat16), flat(), flat(), state(jnp.bfloat16), state(jnp.bfloat16), state(jnp.bfloat16),
            state(jnp.float32), state(jnp.float32),
        ],
        compiler_params=pltpu.CompilerParams(dimension_semantics=("arbitrary",), vmem_limit_bytes=60 * 2**20),
        cost_estimate=pl.CostEstimate(flops=54_000_000_000, bytes_accessed=30_000_000, transcendentals=5_000_000),
        name="layer_backward",
    )(h, dy, both, both, down)


def place(ny, nz):
    s = lax.axis_index("s")
    return s // (2 * nz), lax.rem(s // 2, nz), lax.rem(s, 2)


def greet(peers):
    barrier = pltpu.get_barrier_semaphore()
    for peer in peers:
        pl.semaphore_signal(barrier, inc=1, device_id=peer, device_id_type=pl.DeviceIdType.MESH)
    pl.semaphore_wait(barrier, len(peers))


def remote(src, dst, send, recv, peer):
    return pltpu.make_async_remote_copy(
        src_ref=src, dst_ref=dst, send_sem=send, recv_sem=recv, device_id=peer, device_id_type=pl.DeviceIdType.MESH
    )


def ring(axis, y, z, c, ny, nz):
    n, pos = (ny, y) if axis == "y" else (nz, z)

    def at(k):
        return {"s": ((k * nz + z) if axis == "y" else (y * nz + k)) * 2 + c}

    return n, pos, (at(lax.rem(pos + 1, n)), at(lax.rem(pos + n - 1, n)))


def tile_of(ref, kind, s, first=0, count=40):
    if kind:
        return ref.at[:, pl.ds(pl.multiple_of(s * 40 + first, 8), count), :]
    width = ref.shape[2] // 4
    row, column = pl.multiple_of((s // 4) * 40 + first, 8), pl.multiple_of(lax.rem(s, 4) * width, 128)
    return ref.at[:, pl.ds(row, count), pl.ds(column, width)]


def loop(count, body):
    def run(i, _):
        body(i)
        return 0

    lax.fori_loop(0, count, run, 0)


PARTS = ((0, EDGE), (EDGE, 40 - EDGE))
WHOLE = (0, 40)


def gather_kernel(ny, nz, both_ref, down_ref, both_out, down_out, own_sem, pair_send, pair_recv, send1, recv1, send2, recv2):
    blocks, outs = (both_ref, down_ref), (both_out, down_out)
    y, z, c = place(ny, nz)
    me = (y * nz + z) * 2 + c
    partner = {"s": (y * nz + z) * 2 + (1 - c)}
    greet([partner, *ring("y", y, z, c, ny, nz)[2], *ring("z", y, z, c, ny, nz)[2]])
    own = [pltpu.make_async_copy(blocks[i], tile_of(outs[i], i, me), own_sem.at[i]) for i in range(2)]
    for copy in own:
        copy.start()
    for copy in own:
        copy.wait()

    def handed(yy, zz, core):
        at = yy * nz + zz
        refs = [tile_of(outs[i], i, at * 2 + core) for i in range(2)]
        return [remote(refs[i], refs[i], pair_send.at[at, i], pair_recv.at[at, i], partner) for i in range(2)]

    def hand(yy, zz):
        for copy in handed(yy, zz, c):
            copy.start()

    hand(y, z)

    def phase(axis, where, subs, send, recv):
        n, pos, to = ring(axis, y, z, c, ny, nz)
        h = n // 2

        def copies(d, t, j, ago):
            origin = lax.rem(pos + n - ago, n) if d == 0 else lax.rem(pos + ago, n)
            yy, zz = where(origin, j)
            first, rows = PARTS[d] if t == h - 1 else WHOLE
            refs = [tile_of(outs[i], i, (yy * nz + zz) * 2 + c, first, rows) for i in range(2)]
            return [remote(refs[i], refs[i], send.at[d, t, j, i], recv.at[d, t, j, i], to[d]) for i in range(2)], yy, zz

        for t in range(h):
            def advance(j, t=t):
                for d in (0, 1):
                    if t:
                        came, yy, zz = copies(d, t - 1, j, t)
                        for copy in came:
                            copy.wait_recv()
                    for copy in copies(d, t, j, t)[0]:
                        copy.start()
                    if t:
                        hand(yy, zz)

            loop(subs, advance)

        def last(j):
            for d in (0, 1):
                came, yy, zz = copies(d, h - 1, j, h)
                for copy in came:
                    copy.wait_recv()
            hand(yy, zz)

        loop(subs, last)

        def settle():
            def one(j):
                for t in range(h):
                    for d in (0, 1):
                        for copy in copies(d, t, j, t)[0]:
                            copy.wait_send()

            loop(subs, one)

        return settle

    @pl.when(c == 0)
    def _():
        settle1 = phase("y", lambda k, j: (k, z), 1, send1, recv1)
        settle2 = phase("z", lambda k, j: (j, k), ny, send2, recv2)
        settle1()
        settle2()

    @pl.when(c == 1)
    def _():
        settle1 = phase("z", lambda k, j: (y, k), 1, send1, recv1)
        settle2 = phase("y", lambda k, j: (k, j), nz, send2, recv2)
        settle1()
        settle2()

    def settle(i):
        for copy in handed(i // nz, lax.rem(i, nz), c):
            copy.wait_send()
        for copy in handed(i // nz, lax.rem(i, nz), 1 - c):
            copy.wait_recv()

    loop(ny * nz, settle)


def gathered(both, down, ny=NY, nz=NZ):
    dma = pltpu.SemaphoreType.DMA
    wide, tall = ((both.shape[0], ny * nz * 20, 4 * both.shape[2]), (down.shape[0], ny * nz * 80, down.shape[2]))
    return pl.pallas_call(
        functools.partial(gather_kernel, ny, nz),
        out_shape=[jax.ShapeDtypeStruct(shape, both.dtype) for shape in (wide, tall)],
        in_specs=[pl.BlockSpec(memory_space=pltpu.VMEM)] * 2,
        out_specs=[pl.BlockSpec(memory_space=pl.ANY)] * 2,
        scratch_shapes=[
            dma((2,)), dma((ny * nz, 2)), dma((ny * nz, 2)),
            dma((2, 4, 1, 2)), dma((2, 4, 1, 2)), dma((2, 4, 8, 2)), dma((2, 4, 8, 2)),
        ],
        compiler_params=pltpu.CompilerParams(collective_id=1, has_side_effects=True, vmem_limit_bytes=60 * 2**20),
        cost_estimate=pl.CostEstimate(flops=20_000_000_000, bytes_accessed=10_000_000, transcendentals=0),
        name="gather_plane",
    )(both, down)


def add(into, block, first=0, count=40):
    def one(i):
        at = pl.ds(first, count)
        into[i, at, :] = (into[i, at, :].astype(jnp.float32) + block[i, at, :].astype(jnp.float32)).astype(into.dtype)

    loop(3, one)


def over_planes(out, copies, nx):
    def one(i):
        total = copies[0, i].astype(jnp.float32)
        for k in range(1, nx):
            total += copies[k, i].astype(jnp.float32)
        out[i] = total.astype(out.dtype)

    loop(3, one)


def spread(source, copies, send, recv, nx):
    x = lax.axis_index("r")
    return [remote(source, copies.at[x], send.at[k - 1], recv.at[k - 1], {"r": lax.rem(x + k, nx)}) for k in range(1, nx)]


def keep(source, copies):
    x = lax.axis_index("r")

    def one(i):
        copies[x, i] = source[i]

    loop(3, one)


def reduce_kernel(nx, ny, nz, both_ref, down_ref, out_ref, mine, theirs, arrivals1, arrivals2, copies, own_sem,
                  pair_send, pair_recv, send1, recv1, send2, recv2, xsend, xrecv):
    grads, parts = (both_ref, down_ref), (pl.ds(0, 2), pl.ds(2, 1))
    x = lax.axis_index("r")
    y, z, c = place(ny, nz)
    partner = {"s": (y * nz + z) * 2 + (1 - c)}
    planes = [{"r": lax.rem(x + k, nx)} for k in range(1, nx)]
    greet([partner, *ring("y", y, z, c, ny, nz)[2], *ring("z", y, z, c, ny, nz)[2], *planes])

    def own(yy, zz):
        at = yy * nz + zz
        return [
            pltpu.make_async_copy(tile_of(grads[i], i, at * 2 + c), mine.at[yy, zz, parts[i]], own_sem.at[at, i])
            for i in range(2)
        ]

    def pair(yy, zz, core):
        at = yy * nz + zz
        return [
            remote(
                tile_of(grads[i], i, at * 2 + core), theirs.at[yy, zz, parts[i]], pair_send.at[at, i], pair_recv.at[at, i], partner
            )
            for i in range(2)
        ]

    def needed(n, pos):
        h = n // 2
        offsets = [h]
        for t in range(1, h):
            offsets += [h - t, n - h + t]
        return [lax.rem(pos + k, n) for k in [*offsets, 0]]

    def begin(copies):
        for copy in copies:
            copy.start()

    @pl.when(c == 0)
    def _():
        for k in needed(ny, y):
            loop(nz, lambda j, k=k: begin(pair(k, j, 1)))
        for k in needed(nz, z):
            loop(ny, lambda j, k=k: begin(own(j, k)))

    @pl.when(c == 1)
    def _():
        for k in needed(nz, z):
            loop(ny, lambda j, k=k: begin(pair(j, k, 0)))
        for k in needed(ny, y):
            loop(nz, lambda j, k=k: begin(own(k, j)))

    def both(yy, zz):
        for copy in own(yy, zz):
            copy.wait()
        for copy in pair(yy, zz, 1 - c):
            copy.wait_recv()
        add(mine.at[yy, zz], theirs.at[yy, zz])

    def phase(axis, block, subs, ready, arrivals, send, recv):
        n, pos, to = ring(axis, y, z, c, ny, nz)
        h = n // 2

        def rows_of(ref, d, t):
            return ref.at[:, pl.ds(*PARTS[d])] if t == 0 else ref

        def place_of(d, t):
            return lax.rem(pos + h - t, n) if d == 0 else lax.rem(pos + n - h + t, n)

        def out(d, t, j):
            return remote(
                rows_of(block(place_of(d, t), j), d, t), rows_of(arrivals.at[d, t * subs + j], d, t),
                send.at[d, t, j], recv.at[d, t, j], to[d],
            )

        def arrived(d, t, j, into):
            landed = arrivals.at[d, t * subs + j]
            part = rows_of(landed, d, t)
            remote(part, part, send.at[d, t, j], recv.at[d, t, j], to[d]).wait_recv()
            add(into, landed, *(PARTS[d] if t == 0 else WHOLE))

        for t in range(h):
            def advance(j, t=t):
                for d in (0, 1):
                    if t or d == 0:
                        ready(place_of(d, t), j)
                    if t:
                        arrived(d, t - 1, j, block(place_of(d, t), j))
                    out(d, t, j).start()

            loop(subs, advance)

        def last(j):
            ready(pos, j)
            for d in (0, 1):
                arrived(d, h - 1, j, block(pos, j))

        loop(subs, last)

        def settle():
            def one(j):
                for t in range(h):
                    for d in (0, 1):
                        out(d, t, j).wait_send()

            loop(subs, one)

        return settle

    def done(k, j):
        pass

    @pl.when(c == 0)
    def _():
        settle1 = phase("z", lambda k, j: mine.at[j, k], ny, lambda k, j: both(j, k), arrivals1, send1, recv1)
        settle2 = phase("y", lambda k, j: mine.at[k, z], 1, done, arrivals2, send2, recv2)
        settle1()
        settle2()

    @pl.when(c == 1)
    def _():
        settle1 = phase("y", lambda k, j: mine.at[k, j], nz, lambda k, j: both(k, j), arrivals1, send1, recv1)
        settle2 = phase("z", lambda k, j: mine.at[y, k], 1, done, arrivals2, send2, recv2)
        settle1()
        settle2()

    last = spread(mine.at[y, z], copies, xsend, xrecv, nx)
    for copy in last:
        copy.start()
    keep(mine.at[y, z], copies)
    for copy in last:
        copy.wait()
    over_planes(out_ref, copies, nx)

    def settle(i):
        for copy in pair(i // nz, lax.rem(i, nz), 1 - c):
            copy.wait_send()

    loop(ny * nz, settle)


def reduced(both, down, nx, ny=NY, nz=NZ):
    width = down.shape[2]
    dma = pltpu.SemaphoreType.DMA
    vmem = lambda *lead: pltpu.VMEM((*lead, 3, 40, width), jnp.bfloat16)
    return pl.pallas_call(
        functools.partial(reduce_kernel, nx, ny, nz),
        out_shape=jax.ShapeDtypeStruct((3, 40, width), jnp.bfloat16),
        in_specs=[pl.BlockSpec(memory_space=pl.ANY)] * 2,
        out_specs=pl.BlockSpec(memory_space=pltpu.VMEM),
        scratch_shapes=[
            vmem(ny, nz), vmem(ny, nz), vmem(2, ny * nz // 2), vmem(2, max(ny, nz) // 2), vmem(nx),
            dma((ny * nz, 2)), dma((ny * nz, 2)), dma((ny * nz, 2)),
            dma((2, 4, 8)), dma((2, 4, 8)), dma((2, 4, 1)), dma((2, 4, 1)), dma((max(nx - 1, 1),)), dma((max(nx - 1, 1),)),
        ],
        compiler_params=pltpu.CompilerParams(collective_id=2, has_side_effects=True, vmem_limit_bytes=60 * 2**20),
        cost_estimate=pl.CostEstimate(flops=40_000_000_000, bytes_accessed=20_000_000, transcendentals=0),
        name="reduce_all",
    )(both, down)


def planes_kernel(nx, b_ref, out_ref, copies, send, recv):
    x = lax.axis_index("r")
    greet([{"r": lax.rem(x + k, nx)} for k in range(1, nx)])
    sent = spread(b_ref, copies, send, recv, nx)
    for copy in sent:
        copy.start()
    keep(b_ref, copies)
    for copy in sent:
        copy.wait()
    over_planes(out_ref, copies, nx)


def across_planes(block, nx):
    dma = pltpu.SemaphoreType.DMA((nx - 1,))
    return pl.pallas_call(
        functools.partial(planes_kernel, nx),
        out_shape=jax.ShapeDtypeStruct(block.shape, block.dtype),
        in_specs=[pl.BlockSpec(memory_space=pltpu.VMEM)],
        out_specs=pl.BlockSpec(memory_space=pltpu.VMEM),
        scratch_shapes=[pltpu.VMEM((nx, *block.shape), block.dtype), dma, dma],
        compiler_params=pltpu.CompilerParams(collective_id=3, has_side_effects=True),
        cost_estimate=pl.CostEstimate(flops=5_000_000_000, bytes_accessed=1_000_000, transcendentals=0),
        name="across_planes",
    )(block)


def solution(mesh):
    nx = mesh.shape["r"]
    shards = mesh.shape["s"]
    fours = [[4 * g + m for m in range(4)] for g in range(shards // 4)]

    def step(x, dy, w_gate, w_up, w_down):
        rows = jnp.stack([w_gate, w_up], 1).reshape(2, 2, 10, 4, 640)
        rows = lax.all_to_all(rows, "s", 3, 2, axis_index_groups=fours, tiled=True).reshape(2, 2, 40, 640)
        both, down = gathered(rows.reshape(4, 40, 640), w_down)
        h0 = x[0]
        h1 = forward(h0, 0, both, down)
        by_both, by_down, by_h = backward(h1, dy[0], 1, both, down)
        parts = by_both.reshape(2, shards // 4, 40, 4, 640).transpose(1, 3, 0, 2, 4).reshape(shards, 80, 640)
        terms = jnp.concatenate([parts, by_down.reshape(shards, 40, 640)], 1).reshape(-1, 640)
        second = lax.psum_scatter(terms, "s", scatter_dimension=0, tiled=True).reshape(3, 40, 640)
        by_both, by_down, by_x = backward(h0, by_h, 0, both, down)
        one = reduced(by_both, by_down, nx)
        second, one = lax.optimization_barrier((second, one))
        both = jnp.stack([one, across_planes(second, nx)])
        rows = both[:, :2].reshape(2, 2, 40, 1, 640)
        rows = lax.all_to_all(rows, "s", 2, 3, axis_index_groups=fours, tiled=True).reshape(2, 2, 10, 2560)
        return by_x[None], rows[:, 0], rows[:, 1], both[:, 2]

    states, cut = P(("rep", "r", "s"), None, None), P(None, "s", None)
    return jax.shard_map(
        step,
        mesh=mesh,
        in_specs=(states, states) + (cut,) * 3,
        out_specs=(states,) + (P("rep", "s", None),) * 3,
        check_vma=False,
    )
```

```python
import functools

import jax
import jax.numpy as jnp
from jax import lax
from jax.experimental import pallas as pl
from jax.experimental.pallas import tpu as pltpu
from jax.sharding import PartitionSpec as P

NY, NZ = 4, 8
EDGE = 16


def scale_of(wide):
    return lax.rsqrt(jnp.mean(wide**2, -1, keepdims=True) + 1e-6)


def dot(a, b):
    return jnp.dot(a, b, preferred_element_type=jnp.float32)


def dot_t(a, b):
    return lax.dot_general(a, b, (((1,), (1,)), ((), ())), preferred_element_type=jnp.float32)


def tiles(count, size, body, unroll=False):
    def run(i, _):
        body(pl.ds(pl.multiple_of(i * size, size), size))
        return 0

    lax.fori_loop(0, count // size, run, 0, unroll=unroll)


def forward_kernel(steps, tile, h_ref, g_ref, u_ref, d_ref, y_ref, a_ref, total):
    q = pl.program_id(0)
    tokens = h_ref.shape[0]

    @pl.when(q == 0)
    def _():
        def start(at):
            wide = h_ref[at, :].astype(jnp.float32)
            a_ref[at, :] = (wide * scale_of(wide)).astype(jnp.bfloat16)
            total[at, :] = jnp.zeros((256, h_ref.shape[1]), jnp.float32)

        tiles(tokens, 256, start)

    def main(at):
        a = a_ref[at, :]
        gate, up = dot(a, g_ref[...]), dot(a, u_ref[...])
        act = (gate * jax.nn.sigmoid(gate) * up).astype(jnp.bfloat16)
        total[at, :] += dot(act, d_ref[...])

    tiles(tokens, tile, main)

    @pl.when(q == steps - 1)
    def _():
        def end(at):
            y_ref[at, :] = h_ref[at, :] + total[at, :].astype(jnp.bfloat16)

        tiles(tokens, 256, end)


def forward(h, number, both, down, tile=1024, cut=512):
    tokens, d = h.shape
    steps = both.shape[2] // cut
    whole = pl.BlockSpec((tokens, d), lambda q: (0, 0), pipeline_mode=pl.Buffered(1))
    gate_at = pl.BlockSpec((None, d, cut), lambda q: (2 * number, 0, q))
    up_at = pl.BlockSpec((None, d, cut), lambda q: (2 * number + 1, 0, q))
    down_at = pl.BlockSpec((None, cut, d), lambda q: (number, q, 0))
    return pl.pallas_call(
        functools.partial(forward_kernel, steps, tile),
        grid=(steps,),
        out_shape=jax.ShapeDtypeStruct((tokens, d), jnp.bfloat16),
        in_specs=[whole, gate_at, up_at, down_at],
        out_specs=whole,
        scratch_shapes=[pltpu.VMEM((tokens, d), jnp.bfloat16), pltpu.VMEM((tokens, d), jnp.float32)],
        compiler_params=pltpu.CompilerParams(dimension_semantics=("arbitrary",), vmem_limit_bytes=48 * 2**20),
        cost_estimate=pl.CostEstimate(flops=20_000_000_000, bytes_accessed=15_000_000, transcendentals=5_000_000),
        name="layer_forward",
    )(h, both, both, down)


def backward_kernel(steps, tile, h_ref, dy_ref, g_ref, u_ref, d_ref, by_both, by_d, by_h,
                    a_ref, at_ref, dyt_ref, act_ref, dgate_ref, dup_ref, total_g, total_u):
    q = pl.program_id(0)
    tokens, d = h_ref.shape

    @pl.when(q == 0)
    def _():
        def start(at):
            wide = h_ref[at, :].astype(jnp.float32)
            a = (wide * scale_of(wide)).astype(jnp.bfloat16)
            a_ref[at, :] = a
            at_ref[:, at] = a.T
            dyt_ref[:, at] = dy_ref[at, :].T
            total_g[at, :] = jnp.zeros((256, d), jnp.float32)
            total_u[at, :] = jnp.zeros((256, d), jnp.float32)

        tiles(tokens, 256, start)

    def main(at):
        a = a_ref[at, :]
        gate, up = dot(a, g_ref[...]), dot(a, u_ref[...])
        dact = dot_t(dy_ref[at, :], d_ref[...]).astype(jnp.bfloat16).astype(jnp.float32)
        s = jax.nn.sigmoid(gate)
        silu = gate * s
        act_ref[at, :] = (silu * up).astype(jnp.bfloat16)
        dup = (dact * silu).astype(jnp.bfloat16)
        dgate = (dact * up * (s + silu * (1.0 - s))).astype(jnp.bfloat16)
        dup_ref[at, :] = dup
        dgate_ref[at, :] = dgate
        total_g[at, :] += dot_t(dgate, g_ref[...])
        total_u[at, :] += dot_t(dup, u_ref[...])

    tiles(tokens, tile, main)

    by_d[...] = dot(dyt_ref[...], act_ref[...]).T.astype(jnp.bfloat16)
    by_both[0] = dot(at_ref[...], dgate_ref[...]).astype(jnp.bfloat16)
    by_both[1] = dot(at_ref[...], dup_ref[...]).astype(jnp.bfloat16)

    @pl.when(q == steps - 1)
    def _():
        def end(at):
            wide = h_ref[at, :].astype(jnp.float32)
            scale = scale_of(wide)
            da = (total_g[at, :].astype(jnp.bfloat16) + total_u[at, :].astype(jnp.bfloat16)).astype(jnp.float32)
            along = jnp.sum(da * wide, -1, keepdims=True) * (scale * scale * scale) * (1.0 / d)
            by_h[at, :] = dy_ref[at, :] + (da * scale - wide * along).astype(jnp.bfloat16)

        tiles(tokens, 256, end)


def backward(h, dy, number, both, down, tile=1024, cut=512):
    tokens, d = h.shape
    steps = both.shape[2] // cut
    whole = pl.BlockSpec((tokens, d), lambda q: (0, 0), pipeline_mode=pl.Buffered(1))
    gate_at = pl.BlockSpec((None, d, cut), lambda q: (2 * number, 0, q))
    up_at = pl.BlockSpec((None, d, cut), lambda q: (2 * number + 1, 0, q))
    down_at = pl.BlockSpec((None, cut, d), lambda q: (number, q, 0))
    like = lambda v, count: jax.ShapeDtypeStruct((count, *v.shape[1:]), v.dtype)
    state = lambda t: pltpu.VMEM((tokens, d), t)
    hidden = lambda: pltpu.VMEM((tokens, cut), jnp.bfloat16)
    flat = lambda: pltpu.VMEM((d, tokens), jnp.bfloat16)
    return pl.pallas_call(
        functools.partial(backward_kernel, steps, tile),
        grid=(steps,),
        out_shape=(like(both, 2), like(down, 1), jax.ShapeDtypeStruct(h.shape, h.dtype)),
        in_specs=[whole, whole, gate_at, up_at, down_at],
        out_specs=(pl.BlockSpec((2, d, cut), lambda q: (0, 0, q)), pl.BlockSpec((None, cut, d), lambda q: (0, q, 0)), whole),
        scratch_shapes=[
            state(jnp.bfloat16), flat(), flat(), hidden(), hidden(), hidden(),
            state(jnp.float32), state(jnp.float32),
        ],
        compiler_params=pltpu.CompilerParams(dimension_semantics=("arbitrary",), vmem_limit_bytes=60 * 2**20),
        cost_estimate=pl.CostEstimate(flops=54_000_000_000, bytes_accessed=30_000_000, transcendentals=5_000_000),
        name="layer_backward",
    )(h, dy, both, both, down)


def place(ny, nz):
    s = lax.axis_index("s")
    return s // (2 * nz), lax.rem(s // 2, nz), lax.rem(s, 2)


def greet(peers):
    barrier = pltpu.get_barrier_semaphore()
    for peer in peers:
        pl.semaphore_signal(barrier, inc=1, device_id=peer, device_id_type=pl.DeviceIdType.MESH)
    pl.semaphore_wait(barrier, len(peers))


def remote(src, dst, send, recv, peer):
    return pltpu.make_async_remote_copy(
        src_ref=src, dst_ref=dst, send_sem=send, recv_sem=recv, device_id=peer, device_id_type=pl.DeviceIdType.MESH
    )


def ring(axis, y, z, c, ny, nz):
    n, pos = (ny, y) if axis == "y" else (nz, z)

    def at(k):
        return {"s": ((k * nz + z) if axis == "y" else (y * nz + k)) * 2 + c}

    return n, pos, (at(lax.rem(pos + 1, n)), at(lax.rem(pos + n - 1, n)))


def tile_of(ref, kind, s, first=0, count=40):
    if kind:
        return ref.at[:, pl.ds(pl.multiple_of(s * 40 + first, 8), count), :]
    width = ref.shape[2] // 4
    row, column = pl.multiple_of((s // 4) * 40 + first, 8), pl.multiple_of(lax.rem(s, 4) * width, 128)
    return ref.at[:, pl.ds(row, count), pl.ds(column, width)]


def loop(count, body):
    def run(i, _):
        body(i)
        return 0

    lax.fori_loop(0, count, run, 0)


PARTS = ((0, EDGE), (EDGE, 40 - EDGE))
WHOLE = (0, 40)


def gather_kernel(ny, nz, both_ref, down_ref, both_out, down_out, own_sem, pair_send, pair_recv, send1, recv1, send2, recv2):
    blocks, outs = (both_ref, down_ref), (both_out, down_out)
    y, z, c = place(ny, nz)
    me = (y * nz + z) * 2 + c
    partner = {"s": (y * nz + z) * 2 + (1 - c)}
    greet([partner, *ring("y", y, z, c, ny, nz)[2], *ring("z", y, z, c, ny, nz)[2]])
    own = [pltpu.make_async_copy(blocks[i], tile_of(outs[i], i, me), own_sem.at[i]) for i in range(2)]
    for copy in own:
        copy.start()
    for copy in own:
        copy.wait()

    def handed(yy, zz, core):
        at = yy * nz + zz
        refs = [tile_of(outs[i], i, at * 2 + core) for i in range(2)]
        return [remote(refs[i], refs[i], pair_send.at[at, i], pair_recv.at[at, i], partner) for i in range(2)]

    def hand(yy, zz):
        for copy in handed(yy, zz, c):
            copy.start()

    hand(y, z)

    def phase(axis, where, subs, send, recv):
        n, pos, to = ring(axis, y, z, c, ny, nz)
        h = n // 2

        def copies(d, t, j, ago):
            origin = lax.rem(pos + n - ago, n) if d == 0 else lax.rem(pos + ago, n)
            yy, zz = where(origin, j)
            first, rows = PARTS[d] if t == h - 1 else WHOLE
            refs = [tile_of(outs[i], i, (yy * nz + zz) * 2 + c, first, rows) for i in range(2)]
            return [remote(refs[i], refs[i], send.at[d, t, j, i], recv.at[d, t, j, i], to[d]) for i in range(2)], yy, zz

        for t in range(h):
            def advance(j, t=t):
                for d in (0, 1):
                    if t:
                        came, yy, zz = copies(d, t - 1, j, t)
                        for copy in came:
                            copy.wait_recv()
                    for copy in copies(d, t, j, t)[0]:
                        copy.start()
                    if t:
                        hand(yy, zz)

            loop(subs, advance)

        def last(j):
            for d in (0, 1):
                came, yy, zz = copies(d, h - 1, j, h)
                for copy in came:
                    copy.wait_recv()
            hand(yy, zz)

        loop(subs, last)

        def settle():
            def one(j):
                for t in range(h):
                    for d in (0, 1):
                        for copy in copies(d, t, j, t)[0]:
                            copy.wait_send()

            loop(subs, one)

        return settle

    @pl.when(c == 0)
    def _():
        settle1 = phase("y", lambda k, j: (k, z), 1, send1, recv1)
        settle2 = phase("z", lambda k, j: (j, k), ny, send2, recv2)
        settle1()
        settle2()

    @pl.when(c == 1)
    def _():
        settle1 = phase("z", lambda k, j: (y, k), 1, send1, recv1)
        settle2 = phase("y", lambda k, j: (k, j), nz, send2, recv2)
        settle1()
        settle2()

    def settle(i):
        for copy in handed(i // nz, lax.rem(i, nz), c):
            copy.wait_send()
        for copy in handed(i // nz, lax.rem(i, nz), 1 - c):
            copy.wait_recv()

    loop(ny * nz, settle)


def gathered(both, down, ny=NY, nz=NZ):
    dma = pltpu.SemaphoreType.DMA
    wide, tall = ((both.shape[0], ny * nz * 20, 4 * both.shape[2]), (down.shape[0], ny * nz * 80, down.shape[2]))
    return pl.pallas_call(
        functools.partial(gather_kernel, ny, nz),
        out_shape=[jax.ShapeDtypeStruct(shape, both.dtype) for shape in (wide, tall)],
        in_specs=[pl.BlockSpec(memory_space=pltpu.VMEM)] * 2,
        out_specs=[pl.BlockSpec(memory_space=pl.ANY)] * 2,
        scratch_shapes=[
            dma((2,)), dma((ny * nz, 2)), dma((ny * nz, 2)),
            dma((2, 4, 1, 2)), dma((2, 4, 1, 2)), dma((2, 4, 8, 2)), dma((2, 4, 8, 2)),
        ],
        compiler_params=pltpu.CompilerParams(collective_id=1, has_side_effects=True, vmem_limit_bytes=60 * 2**20),
        cost_estimate=pl.CostEstimate(flops=20_000_000_000, bytes_accessed=10_000_000, transcendentals=0),
        name="gather_plane",
    )(both, down)


def add(into, block, first=0, count=40):
    def one(i):
        at = pl.ds(first, count)
        into[i, at, :] = (into[i, at, :].astype(jnp.float32) + block[i, at, :].astype(jnp.float32)).astype(into.dtype)

    loop(3, one)


def over_planes(out, copies, nx):
    def one(i):
        total = copies[0, i].astype(jnp.float32)
        for k in range(1, nx):
            total += copies[k, i].astype(jnp.float32)
        out[i] = total.astype(out.dtype)

    loop(3, one)


def spread(source, copies, send, recv, nx):
    x = lax.axis_index("r")
    return [remote(source, copies.at[x], send.at[k - 1], recv.at[k - 1], {"r": lax.rem(x + k, nx)}) for k in range(1, nx)]


def keep(source, copies):
    x = lax.axis_index("r")

    def one(i):
        copies[x, i] = source[i]

    loop(3, one)


def reduce_kernel(nx, ny, nz, both_ref, down_ref, out_ref, mine, theirs, arrivals1, arrivals2, copies, own_sem,
                  pair_send, pair_recv, send1, recv1, send2, recv2, xsend, xrecv):
    grads, parts = (both_ref, down_ref), (pl.ds(0, 2), pl.ds(2, 1))
    x = lax.axis_index("r")
    y, z, c = place(ny, nz)
    partner = {"s": (y * nz + z) * 2 + (1 - c)}
    planes = [{"r": lax.rem(x + k, nx)} for k in range(1, nx)]
    greet([partner, *ring("y", y, z, c, ny, nz)[2], *ring("z", y, z, c, ny, nz)[2], *planes])

    def own(yy, zz):
        at = yy * nz + zz
        return [
            pltpu.make_async_copy(tile_of(grads[i], i, at * 2 + c), mine.at[yy, zz, parts[i]], own_sem.at[at, i])
            for i in range(2)
        ]

    def pair(yy, zz, core):
        at = yy * nz + zz
        return [
            remote(
                tile_of(grads[i], i, at * 2 + core), theirs.at[yy, zz, parts[i]], pair_send.at[at, i], pair_recv.at[at, i], partner
            )
            for i in range(2)
        ]

    def needed(n, pos):
        h = n // 2
        offsets = [h]
        for t in range(1, h):
            offsets += [h - t, n - h + t]
        return [lax.rem(pos + k, n) for k in [*offsets, 0]]

    def begin(copies):
        for copy in copies:
            copy.start()

    @pl.when(c == 0)
    def _():
        for k in needed(ny, y):
            loop(nz, lambda j, k=k: begin(pair(k, j, 1)))
        for k in needed(nz, z):
            loop(ny, lambda j, k=k: begin(own(j, k)))

    @pl.when(c == 1)
    def _():
        for k in needed(nz, z):
            loop(ny, lambda j, k=k: begin(pair(j, k, 0)))
        for k in needed(ny, y):
            loop(nz, lambda j, k=k: begin(own(k, j)))

    def both(yy, zz):
        for copy in own(yy, zz):
            copy.wait()
        for copy in pair(yy, zz, 1 - c):
            copy.wait_recv()
        add(mine.at[yy, zz], theirs.at[yy, zz])

    def phase(axis, block, subs, ready, arrivals, send, recv):
        n, pos, to = ring(axis, y, z, c, ny, nz)
        h = n // 2

        def rows_of(ref, d, t):
            return ref.at[:, pl.ds(*PARTS[d])] if t == 0 else ref

        def place_of(d, t):
            return lax.rem(pos + h - t, n) if d == 0 else lax.rem(pos + n - h + t, n)

        def out(d, t, j):
            return remote(
                rows_of(block(place_of(d, t), j), d, t), rows_of(arrivals.at[d, t * subs + j], d, t),
                send.at[d, t, j], recv.at[d, t, j], to[d],
            )

        def arrived(d, t, j, into):
            landed = arrivals.at[d, t * subs + j]
            part = rows_of(landed, d, t)
            remote(part, part, send.at[d, t, j], recv.at[d, t, j], to[d]).wait_recv()
            add(into, landed, *(PARTS[d] if t == 0 else WHOLE))

        for t in range(h):
            def advance(j, t=t):
                for d in (0, 1):
                    if t or d == 0:
                        ready(place_of(d, t), j)
                    if t:
                        arrived(d, t - 1, j, block(place_of(d, t), j))
                    out(d, t, j).start()

            loop(subs, advance)

        def last(j):
            ready(pos, j)
            for d in (0, 1):
                arrived(d, h - 1, j, block(pos, j))

        loop(subs, last)

        def settle():
            def one(j):
                for t in range(h):
                    for d in (0, 1):
                        out(d, t, j).wait_send()

            loop(subs, one)

        return settle

    def done(k, j):
        pass

    @pl.when(c == 0)
    def _():
        settle1 = phase("z", lambda k, j: mine.at[j, k], ny, lambda k, j: both(j, k), arrivals1, send1, recv1)
        settle2 = phase("y", lambda k, j: mine.at[k, z], 1, done, arrivals2, send2, recv2)
        settle1()
        settle2()

    @pl.when(c == 1)
    def _():
        settle1 = phase("y", lambda k, j: mine.at[k, j], nz, lambda k, j: both(k, j), arrivals1, send1, recv1)
        settle2 = phase("z", lambda k, j: mine.at[y, k], 1, done, arrivals2, send2, recv2)
        settle1()
        settle2()

    last = spread(mine.at[y, z], copies, xsend, xrecv, nx)
    for copy in last:
        copy.start()
    keep(mine.at[y, z], copies)
    for copy in last:
        copy.wait()
    over_planes(out_ref, copies, nx)

    def settle(i):
        for copy in pair(i // nz, lax.rem(i, nz), 1 - c):
            copy.wait_send()

    loop(ny * nz, settle)


def reduced(both, down, nx, ny=NY, nz=NZ):
    width = down.shape[2]
    dma = pltpu.SemaphoreType.DMA
    vmem = lambda *lead: pltpu.VMEM((*lead, 3, 40, width), jnp.bfloat16)
    return pl.pallas_call(
        functools.partial(reduce_kernel, nx, ny, nz),
        out_shape=jax.ShapeDtypeStruct((3, 40, width), jnp.bfloat16),
        in_specs=[pl.BlockSpec(memory_space=pl.ANY)] * 2,
        out_specs=pl.BlockSpec(memory_space=pltpu.VMEM),
        scratch_shapes=[
            vmem(ny, nz), vmem(ny, nz), vmem(2, ny * nz // 2), vmem(2, max(ny, nz) // 2), vmem(nx),
            dma((ny * nz, 2)), dma((ny * nz, 2)), dma((ny * nz, 2)),
            dma((2, 4, 8)), dma((2, 4, 8)), dma((2, 4, 1)), dma((2, 4, 1)), dma((max(nx - 1, 1),)), dma((max(nx - 1, 1),)),
        ],
        compiler_params=pltpu.CompilerParams(collective_id=2, has_side_effects=True, vmem_limit_bytes=60 * 2**20),
        cost_estimate=pl.CostEstimate(flops=40_000_000_000, bytes_accessed=20_000_000, transcendentals=0),
        name="reduce_all",
    )(both, down)


def planes_kernel(nx, b_ref, out_ref, copies, send, recv):
    x = lax.axis_index("r")
    greet([{"r": lax.rem(x + k, nx)} for k in range(1, nx)])
    sent = spread(b_ref, copies, send, recv, nx)
    for copy in sent:
        copy.start()
    keep(b_ref, copies)
    for copy in sent:
        copy.wait()
    over_planes(out_ref, copies, nx)


def across_planes(block, nx):
    dma = pltpu.SemaphoreType.DMA((nx - 1,))
    return pl.pallas_call(
        functools.partial(planes_kernel, nx),
        out_shape=jax.ShapeDtypeStruct(block.shape, block.dtype),
        in_specs=[pl.BlockSpec(memory_space=pltpu.VMEM)],
        out_specs=pl.BlockSpec(memory_space=pltpu.VMEM),
        scratch_shapes=[pltpu.VMEM((nx, *block.shape), block.dtype), dma, dma],
        compiler_params=pltpu.CompilerParams(collective_id=3, has_side_effects=True),
        cost_estimate=pl.CostEstimate(flops=5_000_000_000, bytes_accessed=1_000_000, transcendentals=0),
        name="across_planes",
    )(block)


def solution(mesh):
    nx = mesh.shape["r"]
    shards = mesh.shape["s"]
    fours = [[4 * g + m for m in range(4)] for g in range(shards // 4)]

    def step(x, dy, w_gate, w_up, w_down):
        rows = jnp.stack([w_gate, w_up], 1).reshape(2, 2, 10, 4, 640)
        rows = lax.all_to_all(rows, "s", 3, 2, axis_index_groups=fours, tiled=True).reshape(2, 2, 40, 640)
        blocks = lax.all_gather(jnp.concatenate([rows[1].reshape(80, 640), w_down[1]]), "s", axis=0, tiled=True)
        blocks = blocks.reshape(shards // 4, 4, 3, 40, 640)
        both, down = gathered(rows[0], w_down[:1])
        h0 = x[0]
        h1 = forward(h0, 0, both, down)
        next_both = jnp.concatenate([blocks[:, m, :2].swapaxes(0, 1).reshape(2, 640, 640) for m in range(4)], 2)
        next_down = blocks[:, :, 2].reshape(1, 2560, 640)
        by_both, by_down, by_h = backward(h1, dy[0], 0, next_both, next_down)
        parts = [by_both[:, :, 640 * m : 640 * m + 640].reshape(2, shards // 4, 40, 640) for m in range(4)]
        parts = jnp.stack([part[i] for part in parts for i in range(2)], 1).reshape(shards, 2, 40, 640)
        terms = jnp.concatenate([parts, by_down.reshape(shards, 1, 40, 640)], 1).reshape(-1, 640)
        second = lax.psum_scatter(terms, "s", scatter_dimension=0, tiled=True).reshape(3, 40, 640)
        by_both, by_down, by_x = backward(h0, by_h, 0, both, down)
        one = reduced(by_both, by_down, nx)
        second, one = lax.optimization_barrier((second, one))
        both = jnp.stack([one, across_planes(second, nx)])
        rows = both[:, :2].reshape(2, 2, 40, 1, 640)
        rows = lax.all_to_all(rows, "s", 2, 3, axis_index_groups=fours, tiled=True).reshape(2, 2, 10, 2560)
        return by_x[None], rows[:, 0], rows[:, 1], both[:, 2]

    states, cut = P(("rep", "r", "s"), None, None), P(None, "s", None)
    return jax.shard_map(
        step,
        mesh=mesh,
        in_specs=(states, states) + (cut,) * 3,
        out_specs=(states,) + (P("rep", "s", None),) * 3,
        check_vma=False,
    )
```
